32 devices in a mesh: band: 16 (over z, y, x), ga: 2 (over core).
Axes of the slice: x: 2, y: 2, z: 4, core: 2. Of those that a mesh axis runs over, the one named last changes fastest.
Arguments:
- matrix_elements: float32 [2, 4096, 12288], P(None, 'band', 'ga'), may hold values from -6 to 6
- band_index: int32 [4096], P('band'), may hold values from 0 to 1048575
- occupied: int32 [1], replicated, may hold values from 262144 to 786432
- band_weight: float32 [4096], P('band'), may hold values from 0.3 to 3
- coulomb: float32 [12288], replicated, may hold values from 0.2 to 5
Outputs:
- sigma: float32 [12288, 2, 512], P(('ga', 'band'))
The draws below stay inside these ranges and needn't reach their ends.
All inputs are finite; a program needn't handle non-finite values.
Results may differ from the reference program's by a relative error of at most 0.00018.
Values sent between devices are 32-bit elements; how exact they have to be, the bound alone decides.
A program may use at most 192 MiB of HBM per device.

```python
import math
import jax
import jax.numpy as jnp
from jax import lax

NG = 12288
COLS = 512
NB = 4096


def place_ends(drawn, rng, least, top_value):
    index_at = [jax.random.randint(jax.random.fold_in(rng, axis), (), 0, length) for axis, length in enumerate(drawn.shape)]
    widest = drawn.shape.index(max(drawn.shape))
    neighbour = index_at[:widest] + [(index_at[widest] + 1) % drawn.shape[widest]] + index_at[widest + 1:]
    return drawn.at[tuple(index_at)].set(least).at[tuple(neighbour)].set(top_value)


def strengthened(result, own_key, source, target, blocks, factor):
    owner, partner = [(jnp.arange(result.shape[axis_at]) // (result.shape[axis_at] // blocks)).reshape([-1 if axis == axis_at else 1 for axis in range(result.ndim)]) for axis_at in (source, target)]
    chosen = jax.random.permutation(own_key, blocks)[partner]
    strong = (owner == chosen) | (owner == (partner + blocks // 2) % blocks)
    return jnp.where(strong, factor * result, result)


def shard_levels(stream_key, shape, shards, smallest, top_value):
    level, own = 1.0, jax.random.fold_in(stream_key, 6)
    for axis_at, parts in shards:
        draws = jnp.exp(jax.random.uniform(jax.random.fold_in(own, axis_at), (parts,), jnp.float32, smallest / len(shards), top_value / len(shards)))
        level = level * jnp.repeat(draws, shape[axis_at] // parts).reshape([-1 if axis == axis_at else 1 for axis in range(len(shape))])
    return level


def bell_draw_with(stream_key, shape, width, bound, cuts, heavy, dtype=jnp.bfloat16):
    drawn = width * jax.random.normal(stream_key, shape, jnp.float32)
    if cuts:
        drawn = drawn * shard_levels(stream_key, shape, cuts, -0.22, 0.18)
    return jnp.clip(strengthened(drawn, jax.random.fold_in(stream_key, 3), *heavy), -bound, bound).astype(dtype)


def setup_inputs(seed: int = 0) -> dict:
    arg_keys = jax.random.split(jax.random.key(seed), 6)
    return {
        "matrix_elements": bell_draw_with(arg_keys[0], (2, NB, NG), 1.0, 6.0, ((1, 16), (2, 2)), (1, 2, 16, 2.0), jnp.float32),
        "band_index": place_ends(jax.random.randint(arg_keys[1], (NB,), 0, 1048576), jax.random.fold_in(arg_keys[1], 1), 0, 1048575).astype(jnp.int32),
        "occupied": jax.random.randint(arg_keys[2], (1,), 262144, 786433).astype(jnp.int32),
        "band_weight": jnp.clip(jnp.exp(math.log(3.0) - 2.3025851 * jax.random.uniform(arg_keys[3], (NB,), jnp.float32) ** shard_levels(arg_keys[3], (NB,), ((0, 16),), -0.2, 0.2)), 0.3, 3.0),
        "coulomb": jnp.clip(jnp.exp(jax.random.uniform(arg_keys[4], (NG,), jnp.float32, math.log(0.2), math.log(5.0))), 0.2, 5.0),
    }


def reference(matrix_elements, band_index, occupied, band_weight, coulomb):
    occ = (band_index < occupied[0]).astype(jnp.float32)
    coef = (0.5 - occ) * band_weight
    real = matrix_elements[0]
    imag = matrix_elements[1]
    left = jnp.concatenate([coef[:, None] * real, coef[:, None] * imag], 0)
    slab_re = real[:, :COLS]
    slab_im = imag[:, :COLS]
    right = jnp.concatenate([jnp.concatenate([slab_re, slab_im], 1), jnp.concatenate([slab_im, -slab_re], 1)], 0)
    factor = 1.0 / math.sqrt(NB)
    sums = lax.dot_general(left, right, (((0,), (0,)), ((), ())), precision=lax.Precision.HIGHEST, preferred_element_type=jnp.float32) * factor
    square = 2.0 - real * real - imag * imag
    defect = jnp.dot(coef, square, precision=lax.Precision.HIGHEST, preferred_element_type=jnp.float32) * factor
    weight = jnp.sqrt(coulomb[:, None] * coulomb[None, :COLS])
    part_re = weight * (sums[:, :COLS] + 0.5 * (defect[:, None] + defect[None, :COLS]))
    part_im = weight * sums[:, COLS:]
    return jnp.stack([part_re, part_im], 1)
```

```python
import math

import jax
import jax.numpy as jnp
from jax import lax
from jax.sharding import PartitionSpec as P

COLS = 512


def contract(left, right):
    return lax.dot_general(
        left,
        right,
        (((0,), (0,)), ((), ())),
        precision=lax.Precision.HIGH,
        preferred_element_type=jnp.float32,
    )


def right_side(slab):
    return jnp.concatenate(
        [jnp.concatenate([slab[0], slab[1]], 1), jnp.concatenate([slab[1], -slab[0]], 1)], 0
    )


def defects(coef, block):
    return jnp.sum(coef[:, None] * (2.0 - block[0] * block[0] - block[1] * block[1]), 0)


def body(matrix_elements, band_index, occupied, band_weight, coulomb):
    bands_dev = matrix_elements.shape[1]
    half = matrix_elements.shape[2]
    n_band = lax.axis_size("band")
    n_bits = n_band.bit_length() - 1
    rows_dev = half // n_band
    n_ga = lax.axis_size("ga")
    chunks = 3 if rows_dev % 3 == 0 else 1
    width = rows_dev // chunks
    factor = 1.0 / math.sqrt(bands_dev * n_band)
    band_pos = lax.axis_index("band")
    ga_pos = lax.axis_index("ga")
    bits = list(range(n_bits))
    orders = [bits, bits[1:] + bits[:1], bits[2:3] + bits[:2] + bits[3:]][:chunks]

    def swap(x, bit):
        return lax.ppermute(x, "band", [(i, i ^ (1 << bit)) for i in range(n_band)])

    def mine(bit):
        return (band_pos >> bit) & 1

    def pick(x, c, bit, which):
        parts = []
        for d in range(n_band):
            if not (d >> bit) & 1:
                low = d * rows_dev + c * width
                high = (d | (1 << bit)) * rows_dev + c * width
                parts.append(
                    jnp.where(which == 1, x[..., high : high + width], x[..., low : low + width])
                )
        return jnp.concatenate(parts, -1)

    there = [
        swap(pick(matrix_elements, c, order[0], 1 - mine(order[0])), order[0])
        for c, order in enumerate(orders)
    ]

    occ = (band_index < occupied[0]).astype(jnp.float32)
    coef = (0.5 - occ) * band_weight
    first = matrix_elements[:, :, :COLS]
    moved = lax.ppermute(first, "ga", [(0, g) for g in range(1, n_ga)][:1])
    slab = jnp.where(ga_pos == 0, first, moved)
    scaled = coef[None, :, None] * slab
    scaled_there = [swap(scaled, order[0]) for order in orders]
    row_def = defects(coef, matrix_elements)
    col_def = defects(coef, slab)

    sums = []
    for c, order in enumerate(orders):
        bit = order[0]
        rows_here = pick(row_def, c, bit, mine(bit))
        send = jnp.concatenate([pick(row_def, c, bit, 1 - mine(bit)), col_def])
        got = swap(send, bit)
        count = rows_here.shape[0]
        rows_sum = rows_here + got[:count]
        cols_sum = col_def + got[count:]
        here = pick(matrix_elements, c, bit, mine(bit))
        part = contract(here.reshape(2 * bands_dev, count), right_side(scaled))
        part = part + contract(
            there[c].reshape(2 * bands_dev, count), right_side(scaled_there[c])
        )
        extra = 0.5 * (rows_sum[:, None] + cols_sum[None, :])
        part = part + jnp.concatenate([extra, jnp.zeros_like(extra)], 1)
        sums.append(part.reshape((2,) * (n_bits - 1) + (width, 2 * COLS)))

    left = [[b for b in reversed(bits) if b != order[0]] for order in orders]
    for step in range(1, n_bits):
        sent = []
        for c, order in enumerate(orders):
            bit = order[step]
            axis = left[c].index(bit)
            sent.append(
                swap(
                    lax.dynamic_index_in_dim(sums[c], 1 - mine(bit), axis, keepdims=False), bit
                )
            )
        for c, order in enumerate(orders):
            bit = order[step]
            axis = left[c].index(bit)
            keep = lax.dynamic_index_in_dim(sums[c], mine(bit), axis, keepdims=False)
            sums[c] = keep + sent[c]
            left[c].remove(bit)

    total = jnp.concatenate(sums, 0)
    row_coul = lax.dynamic_slice_in_dim(coulomb, ga_pos * half + band_pos * rows_dev, rows_dev, 0)
    weight = factor * jnp.sqrt(row_coul[:, None] * coulomb[None, :COLS])
    return jnp.stack([weight * total[:, :COLS], weight * total[:, COLS:]], 1)


def solution(mesh):
    return jax.shard_map(
        body,
        mesh=mesh,
        in_specs=(P(None, "band", "ga"), P("band"), P(), P("band"), P()),
        out_specs=P(("ga", "band"), None, None),
        check_vma=False,
    )
```

```python
import math

import jax
import jax.numpy as jnp
from jax import lax
from jax.sharding import PartitionSpec as P

COLS = 512


def contract(left, right):
    return lax.dot_general(
        left,
        right,
        (((0,), (0,)), ((), ())),
        precision=lax.Precision.HIGH,
        preferred_element_type=jnp.float32,
    )


def right_side(slab):
    return jnp.concatenate(
        [jnp.concatenate([slab[0], slab[1]], 1), jnp.concatenate([slab[1], -slab[0]], 1)], 0
    )


def defects(coef, block):
    return jnp.sum(coef[:, None] * (2.0 - block[0] * block[0] - block[1] * block[1]), 0)


def body(matrix_elements, band_index, occupied, band_weight, coulomb):
    bands_dev = matrix_elements.shape[1]
    half = matrix_elements.shape[2]
    n_band = lax.axis_size("band")
    n_bits = n_band.bit_length() - 1
    rows_dev = half // n_band
    n_ga = lax.axis_size("ga")
    chunks = 3 if rows_dev % 3 == 0 else 1
    width = rows_dev // chunks
    factor = 1.0 / math.sqrt(bands_dev * n_band)
    band_pos = lax.axis_index("band")
    ga_pos = lax.axis_index("ga")
    bits = list(range(n_bits - 1))
    top = n_band // 2
    firsts = [b % len(bits) for b in range(chunks)]
    streams = [(c, p) for p in range(2) for c in range(chunks)]
    orders = {}
    for c, p in streams:
        rest = bits[firsts[c] + 1 :] + bits[: firsts[c]]
        orders[c, p] = rest[p:] + rest[:p]

    def swap(x, bit):
        return lax.ppermute(x, "band", [(i, i ^ (1 << bit)) for i in range(n_band)])

    def mine(bit):
        return (band_pos >> bit) & 1

    def pick(x, c, p, which):
        bit = firsts[c]
        parts = []
        for d in range(p * top, (p + 1) * top):
            if not (d >> bit) & 1:
                low = d * rows_dev + c * width
                high = (d | (1 << bit)) * rows_dev + c * width
                parts.append(
                    jnp.where(which == 1, x[..., high : high + width], x[..., low : low + width])
                )
        return jnp.concatenate(parts, -1)

    there = {
        (c, p): swap(pick(matrix_elements, c, p, 1 - mine(firsts[c])), firsts[c])
        for c, p in streams
    }

    occ = (band_index < occupied[0]).astype(jnp.float32)
    coef = (0.5 - occ) * band_weight
    first = matrix_elements[:, :, :COLS]
    moved = lax.ppermute(first, "ga", [(0, g) for g in range(1, n_ga)][:1])
    slab = jnp.where(ga_pos == 0, first, moved)
    scaled = coef[None, :, None] * slab
    right = right_side(scaled)
    rights = [right_side(swap(scaled, bit)) for bit in firsts]
    row_def = defects(coef, matrix_elements)
    col_def = defects(coef, slab)

    sums, left = {}, {}
    for c, p in streams:
        bit = firsts[c]
        rows_here = pick(row_def, c, p, mine(bit))
        send = jnp.concatenate([pick(row_def, c, p, 1 - mine(bit)), col_def])
        got = swap(send, bit)
        count = rows_here.shape[0]
        rows_sum = rows_here + got[:count]
        cols_sum = col_def + got[count:]
        here = pick(matrix_elements, c, p, mine(bit))
        part = contract(here.reshape(2 * bands_dev, count), right)
        part = part + contract(there[c, p].reshape(2 * bands_dev, count), rights[c])
        extra = 0.5 * (rows_sum[:, None] + cols_sum[None, :])
        part = part + jnp.concatenate([extra, jnp.zeros_like(extra)], 1)
        sums[c, p] = part.reshape((2,) * (n_bits - 2) + (width, 2 * COLS))
        left[c, p] = [b for b in reversed(bits) if b != bit]

    for step in range(n_bits - 2):
        sent = {}
        for k in streams:
            bit = orders[k][step]
            send = lax.dynamic_index_in_dim(
                sums[k], 1 - mine(bit), left[k].index(bit), keepdims=False
            )
            sent[k] = swap(send, bit)
        for k in streams:
            bit = orders[k][step]
            keep = lax.dynamic_index_in_dim(sums[k], mine(bit), left[k].index(bit), keepdims=False)
            sums[k] = keep + sent[k]
            left[k].remove(bit)

    upper = mine(n_bits - 1) == 1
    last = [swap(jnp.where(upper, sums[c, 0], sums[c, 1]), n_bits - 1) for c in range(chunks)]
    done = [jnp.where(upper, sums[c, 1], sums[c, 0]) + last[c] for c in range(chunks)]
    total = jnp.concatenate(done, 0)
    row_coul = lax.dynamic_slice_in_dim(coulomb, ga_pos * half + band_pos * rows_dev, rows_dev, 0)
    weight = factor * jnp.sqrt(row_coul[:, None] * coulomb[None, :COLS])
    return jnp.stack([weight * total[:, :COLS], weight * total[:, COLS:]], 1)


def solution(mesh):
    return jax.shard_map(
        body,
        mesh=mesh,
        in_specs=(P(None, "band", "ga"), P("band"), P(), P("band"), P()),
        out_specs=P(("ga", "band"), None, None),
        check_vma=False,
    )
```
